8 devices in a mesh: dp: 2 (over z, y), sp: 4 (over x, core).
Axes of the slice: x: 2, y: 2, z: 1, core: 2. Of those that a mesh axis runs over, the one named last changes fastest.
Arguments:
- signal: bfloat16 [65536, 768], P(('dp', 'sp')), parts along dimension 0
- w_first: bfloat16 [8, 256, 2, 128, 128], P(None, 'sp')
- w_second: bfloat16 [8, 256, 2, 128, 128], P(None, 'sp')
Outputs:
- output: bfloat16 [65536, 768], P(('dp', 'sp')), parts along dimension 0
There are 2 independent parts. The reference program is written for one: setup_inputs(seed, part) draws one part's arguments, and reference() takes and returns one part's arrays. A program takes and returns all parts, laid end to end along the dimension named above; an argument that names none is the same for every part.
All inputs are finite; a program needn't handle non-finite values.
Results may differ from the reference program's by a relative error of at most 0.02.
Values are sent between devices in bfloat16 or wider.
A program may use at most 1 GiB of HBM per device.

```python
import jax
import jax.numpy as jnp
import math
from jax import lax

SEQ_LEN = 32768
CHANNELS = 768
BLOCK_SIZE = 128

NUM_BLOCKS = SEQ_LEN // BLOCK_SIZE
STAGES = int(math.log2(NUM_BLOCKS))


def setup_inputs(seed: int = 0, part: int = 0) -> dict:
    key_signal = jax.random.fold_in(jax.random.key(seed + 1), part)
    key_first = jax.random.key(seed + 2)
    key_second = jax.random.key(seed + 3)
    w_shape = (STAGES, NUM_BLOCKS, 2, BLOCK_SIZE, BLOCK_SIZE)
    w_scale = (2 * BLOCK_SIZE) ** -0.5
    signal = jax.random.normal(key_signal, (SEQ_LEN, CHANNELS), jnp.float32)
    w_first = jax.random.normal(key_first, w_shape, jnp.float32) * w_scale
    w_second = jax.random.normal(key_second, w_shape, jnp.float32) * w_scale
    return {"signal": signal.astype(jnp.bfloat16), "w_first": w_first.astype(jnp.bfloat16), "w_second": w_second.astype(jnp.bfloat16)}


def butterfly_stage(act_blocks, weights, distance):
    grouped = act_blocks.reshape(NUM_BLOCKS // (2 * distance), 2, distance, BLOCK_SIZE, act_blocks.shape[2])
    partner = grouped[:, ::-1].reshape(act_blocks.shape)
    paired = jnp.stack([act_blocks, partner], axis=1).astype(jnp.float32)
    mixed = jnp.einsum("ltij,ltjc->lic", weights.astype(jnp.float32), paired)
    return mixed.astype(jnp.bfloat16)


def apply_map(act_blocks, weights, distances):
    for stage, distance in enumerate(distances):
        act_blocks = butterfly_stage(act_blocks, weights[stage], distance)
    return act_blocks


def reference(signal, w_first, w_second):
    col_width = min(CHANNELS, 128)
    col_groups = CHANNELS // col_width
    grouped = signal.reshape(NUM_BLOCKS, BLOCK_SIZE, col_groups, col_width).transpose(2, 0, 1, 3)
    dist_down = [2 ** (STAGES - 1 - level) for level in range(STAGES)]
    dist_up = [2 ** level for level in range(STAGES)]

    def one_group(act_blocks):
        hidden = apply_map(act_blocks, w_first, dist_down)
        hidden = jax.nn.gelu(hidden.astype(jnp.float32), approximate=False).astype(jnp.bfloat16)
        return apply_map(hidden, w_second, dist_up)

    mapped = lax.map(one_group, grouped)
    return mapped.transpose(1, 2, 0, 3).reshape(SEQ_LEN, CHANNELS)
```

```python
import functools

import jax
import jax.numpy as jnp
from jax import lax
from jax.experimental import pallas as pl
from jax.experimental.pallas import tpu as pltpu
from jax.sharding import PartitionSpec as P


CHUNKS = ((0, 256), (256, 256), (512, 128), (640, 128))

ERFC_P = (2.326819970068386e-2, -1.387039388740657e-1, 3.687424674597105e-1, -5.824733027278666e-1, 6.210004621745983e-1,
          -4.944515323274145e-1, 3.404879937665872e-1, -2.741127028184656e-1, 5.638259427386472e-1)
ERFC_R = (-1.047766399936249e1, 1.297719955372516e1, -7.495518717768503e0, 2.921019019210786e0, -1.015265279202700e0,
          4.218463358204948e-1, -2.820767439740514e-1, 5.641895067754075e-1)


def horner(coeffs, y):
    total = jnp.full_like(y, coeffs[0])
    for c in coeffs[1:]:
        total = total * y + c
    return total


def gelu(x):
    a = x * (-(0.5 ** 0.5))
    mag = jnp.abs(a)
    far = jnp.maximum(mag, 1.0)
    q = 1.0 / far
    y = q * q
    poly = jnp.where(far < 2.0, horner(ERFC_P, y), horner(ERFC_R, y))
    tail = jnp.exp(-far * far) * q * poly
    tail = jnp.where(a < 0.0, 2.0 - tail, tail)
    return 0.5 * x * jnp.where(mag < 1.0, 1.0 - lax.erf(a), tail)


def mix(w_own, w_cross, z_own, z_cross):
    weights = jnp.concatenate([w_own, w_cross], axis=1)
    blocks = jnp.concatenate([z_own, z_cross], axis=0)
    return jnp.dot(weights, blocks, preferred_element_type=jnp.float32)


def cross_kernel(blocks, *refs):
    own, partner, w, out = refs[0], refs[1], refs[2], refs[-1]
    size = w.shape[-1]
    for b in range(blocks):
        rows = pl.ds(b * size, size)
        out[rows, :] = mix(w[0, b, 0], w[0, b, 1], own[rows, :], partner[rows, :]).astype(out.dtype)


def cross_stage(own, own_col, partner, weights, stage, width, out_cols, out_col, into=None, blocks=8):
    local, size = weights.shape[1], weights.shape[-1]
    rows = own.shape[0]
    operands = [own, partner, weights]
    in_specs = [
        pl.BlockSpec((blocks * size, width), lambda g: (g, own_col)),
        pl.BlockSpec((blocks * size, width), lambda g: (g, 0)),
        pl.BlockSpec((1, blocks, 2, size, size), lambda g: (stage, g, 0, 0, 0)),
    ]
    aliases = {}
    if into is not None:
        operands.append(into)
        in_specs.append(pl.BlockSpec(memory_space=pl.ANY))
        aliases = {3: 0}
    flops = 4 * rows * size * width
    return pl.pallas_call(
        functools.partial(cross_kernel, blocks),
        grid=(local // blocks,),
        out_shape=jax.ShapeDtypeStruct((rows, out_cols), own.dtype),
        in_specs=in_specs,
        out_specs=pl.BlockSpec((blocks * size, width), lambda g: (g, out_col)),
        input_output_aliases=aliases,
        compiler_params=pltpu.CompilerParams(dimension_semantics=("arbitrary",)),
        cost_estimate=pl.CostEstimate(flops=flops, bytes_accessed=6 * rows * width + 4 * rows * size, transcendentals=0),
        name="cross_stage",
    )(*operands)


def local_kernel(first_steps, own, partner, wf, ws, out, other):
    step = pl.program_id(0)
    local, size = wf.shape[1], wf.shape[-1]

    @pl.when(step == 0)
    def _():
        def body(b, carry):
            rows = pl.ds(pl.multiple_of(b * size, size), size)
            out[rows, :] = mix(wf[0, b, 0], wf[0, b, 1], own[rows, :], partner[rows, :]).astype(out.dtype)
            return carry
        lax.fori_loop(0, local, body, 0, unroll=8)

    def stage(w, src, dst, shift, act):
        def body(p, carry):
            i = lax.shift_left(lax.shift_right_logical(p, shift), shift + 1) + (p & (lax.shift_left(1, shift) - 1))
            j = i + lax.shift_left(1, shift)
            ri = pl.ds(pl.multiple_of(i * size, size), size)
            rj = pl.ds(pl.multiple_of(j * size, size), size)
            zi, zj = src[ri, :], src[rj, :]
            blocks = jnp.concatenate([zi, zj], axis=0)
            weights = jnp.concatenate([
                jnp.concatenate([w[0, i, 0], w[0, i, 1]], axis=1),
                jnp.concatenate([w[0, j, 1], w[0, j, 0]], axis=1),
            ], axis=0)
            mixed = jnp.dot(weights, blocks, preferred_element_type=jnp.float32)
            mixed = mixed.astype(dst.dtype)
            if act:
                mixed = gelu(mixed.astype(jnp.float32)).astype(dst.dtype)
            dst[ri, :] = mixed[:size]
            dst[rj, :] = mixed[size:]
            return carry
        lax.fori_loop(0, local // 2, body, 0, unroll=1 if act else 4)

    odd = (step % 2) == 1

    @pl.when(jnp.logical_and(jnp.logical_and(step >= 1, step < first_steps), odd))
    def _():
        stage(wf, out, other, first_steps - step, False)

    @pl.when(jnp.logical_and(jnp.logical_and(step >= 1, step < first_steps), jnp.logical_not(odd)))
    def _():
        stage(wf, other, out, first_steps - step, False)

    @pl.when(step == first_steps)
    def _():
        if first_steps % 2:
            stage(wf, out, other, 0, True)
        else:
            stage(wf, other, out, 0, True)

    @pl.when(jnp.logical_and(step > first_steps, odd))
    def _():
        stage(ws, out, other, step - first_steps - 1, False)

    @pl.when(jnp.logical_and(step > first_steps, jnp.logical_not(odd)))
    def _():
        stage(ws, other, out, step - first_steps - 1, False)


def local_stages(own, partner, w_first, w_second, skip):
    stages, local, _, size, _ = w_first.shape
    rows, width = own.shape
    first_steps = stages - skip
    steps = 1 + 2 * first_steps
    whole = pl.BlockSpec((rows, width), lambda t: (0, 0))
    w_block = (1, local, 2, size, size)
    flops = 4 * rows * size * width * steps
    return pl.pallas_call(
        functools.partial(local_kernel, first_steps),
        grid=(steps,),
        out_shape=jax.ShapeDtypeStruct((rows, width), own.dtype),
        in_specs=[
            whole,
            whole,
            pl.BlockSpec(w_block, lambda t: (jnp.minimum(t + skip - 1, stages - 1), 0, 0, 0, 0)),
            pl.BlockSpec(w_block, lambda t: (jnp.maximum(t - first_steps - 1, 0), 0, 0, 0, 0)),
        ],
        out_specs=whole,
        scratch_shapes=[pltpu.VMEM((rows, width), own.dtype)],
        compiler_params=pltpu.CompilerParams(dimension_semantics=("arbitrary",), vmem_limit_bytes=60 * 1024 * 1024),
        cost_estimate=pl.CostEstimate(flops=flops, bytes_accessed=6 * rows * width + 4 * rows * size * steps, transcendentals=0),
        name="local_stages",
    )(own, partner, w_first, w_second)


def solution(mesh):
    groups = mesh.shape["sp"]

    def swap(array, dev_step):
        return lax.ppermute(array, "sp", [(device, device ^ dev_step) for device in range(groups)])

    def device_program(signal, w_first, w_second):
        stages, local = w_first.shape[:2]
        cols = signal.shape[1]
        far = (2 ** (stages - 1)) // local
        near = far // 2
        sent = [swap(signal[:, off:off + width], far) for off, width in CHUNKS]
        late = []
        for (off, width), partner in zip(CHUNKS, sent):
            act = cross_stage(signal, off // width, partner, w_first, 0, width, width, 0)
            act = local_stages(act, swap(act, near), w_first, w_second, 2)
            act = cross_stage(act, 0, swap(act, near), w_second, stages - 2, width, width, 0)
            late.append((act, swap(act, far)))
        result = None
        for (off, width), (act, partner) in zip(CHUNKS, late):
            result = cross_stage(act, 0, partner, w_second, stages - 1, width, cols, off // width, into=result)
        return result

    row_spec = P(("dp", "sp"), None)
    weight_spec = P(None, "sp", None, None, None)
    return jax.shard_map(device_program, mesh=mesh, in_specs=(row_spec, weight_spec, weight_spec), out_specs=row_spec, check_vma=False)
```

```python
import functools

import jax
import jax.numpy as jnp
from jax import lax
from jax.experimental import pallas as pl
from jax.experimental.pallas import tpu as pltpu
from jax.sharding import PartitionSpec as P


WIDTH = 256
LAST_PIECES = (32, 16, 16)

ERFC_P = (2.326819970068386e-2, -1.387039388740657e-1, 3.687424674597105e-1, -5.824733027278666e-1, 6.210004621745983e-1,
          -4.944515323274145e-1, 3.404879937665872e-1, -2.741127028184656e-1, 5.638259427386472e-1)
ERFC_R = (-1.047766399936249e1, 1.297719955372516e1, -7.495518717768503e0, 2.921019019210786e0, -1.015265279202700e0,
          4.218463358204948e-1, -2.820767439740514e-1, 5.641895067754075e-1)


def horner(coeffs, y):
    total = jnp.full_like(y, coeffs[0])
    for c in coeffs[1:]:
        total = total * y + c
    return total


def gelu(x):
    a = x * (-(0.5 ** 0.5))
    mag = jnp.abs(a)
    far = jnp.maximum(mag, 1.0)
    q = 1.0 / far
    y = q * q
    poly = jnp.where(far < 2.0, horner(ERFC_P, y), horner(ERFC_R, y))
    tail = jnp.exp(-far * far) * q * poly
    tail = jnp.where(a < 0.0, 2.0 - tail, tail)
    return 0.5 * x * jnp.where(mag < 1.0, 1.0 - lax.erf(a), tail)


def mix(w_own, w_cross, z_own, z_cross):
    weights = jnp.concatenate([w_own, w_cross], axis=1)
    blocks = jnp.concatenate([z_own, z_cross], axis=0)
    return jnp.dot(weights, blocks, preferred_element_type=jnp.float32)


def cross_kernel(blocks, *refs):
    own, partner, w, out = refs[0], refs[1], refs[2], refs[-1]
    size = w.shape[-1]
    for b in range(blocks):
        rows = pl.ds(b * size, size)
        out[rows, :] = mix(w[0, b, 0], w[0, b, 1], own[rows, :], partner[rows, :]).astype(out.dtype)


def cross_stage(own, partner, weights, stage, first, count, width, own_at, partner_at, out_shape, out_at, into=None, after=(), blocks=8):
    size = weights.shape[-1]
    any_space = pl.BlockSpec(memory_space=pl.ANY)

    def spec(at):
        row, col = at
        return pl.BlockSpec((blocks * size, width), lambda g: (row // blocks + g, col))

    operands = [own, partner, weights]
    in_specs = [
        spec(own_at),
        spec(partner_at),
        pl.BlockSpec((1, blocks, 2, size, size), lambda g: (stage, first // blocks + g, 0, 0, 0)),
    ]
    aliases = {}
    if into is not None:
        aliases = {len(operands): 0}
        operands.append(into)
    operands += after
    in_specs += [any_space] * (len(operands) - len(in_specs))
    rows = count * size
    return pl.pallas_call(
        functools.partial(cross_kernel, blocks),
        grid=(count // blocks,),
        out_shape=jax.ShapeDtypeStruct(out_shape, own.dtype),
        in_specs=in_specs,
        out_specs=spec(out_at),
        input_output_aliases=aliases,
        compiler_params=pltpu.CompilerParams(dimension_semantics=("arbitrary",)),
        cost_estimate=pl.CostEstimate(
            flops=4 * rows * size * width, bytes_accessed=6 * rows * width + 4 * rows * size, transcendentals=0),
        name="cross_stage",
    )(*operands)


def local_kernel(first_steps, own, partner, wf, ws, out, other):
    step = pl.program_id(0)
    local, size = wf.shape[1], wf.shape[-1]

    @pl.when(step == 0)
    def _():
        def body(b, carry):
            rows = pl.ds(pl.multiple_of(b * size, size), size)
            out[rows, :] = mix(wf[0, b, 0], wf[0, b, 1], own[rows, :], partner[rows, :]).astype(out.dtype)
            return carry

        lax.fori_loop(0, local, body, 0, unroll=8)

    def stage(w, src, dst, shift, act):
        def body(p, carry):
            i = lax.shift_left(lax.shift_right_logical(p, shift), shift + 1) + (p & (lax.shift_left(1, shift) - 1))
            j = i + lax.shift_left(1, shift)
            ri = pl.ds(pl.multiple_of(i * size, size), size)
            rj = pl.ds(pl.multiple_of(j * size, size), size)
            zi, zj = src[ri, :], src[rj, :]
            blocks = jnp.concatenate([zi, zj], axis=0)
            weights = jnp.concatenate([
                jnp.concatenate([w[0, i, 0], w[0, i, 1]], axis=1),
                jnp.concatenate([w[0, j, 1], w[0, j, 0]], axis=1),
            ], axis=0)
            mixed = jnp.dot(weights, blocks, preferred_element_type=jnp.float32)
            mixed = mixed.astype(dst.dtype)
            if act:
                mixed = gelu(mixed.astype(jnp.float32)).astype(dst.dtype)
            dst[ri, :] = mixed[:size]
            dst[rj, :] = mixed[size:]
            return carry

        lax.fori_loop(0, local // 2, body, 0, unroll=1 if act else 4)

    odd = (step % 2) == 1

    @pl.when(jnp.logical_and(jnp.logical_and(step >= 1, step < first_steps), odd))
    def _():
        stage(wf, out, other, first_steps - step, False)

    @pl.when(jnp.logical_and(jnp.logical_and(step >= 1, step < first_steps), jnp.logical_not(odd)))
    def _():
        stage(wf, other, out, first_steps - step, False)

    @pl.when(step == first_steps)
    def _():
        if first_steps % 2:
            stage(wf, out, other, 0, True)
        else:
            stage(wf, other, out, 0, True)

    @pl.when(jnp.logical_and(step > first_steps, odd))
    def _():
        stage(ws, out, other, step - first_steps - 1, False)

    @pl.when(jnp.logical_and(step > first_steps, jnp.logical_not(odd)))
    def _():
        stage(ws, other, out, step - first_steps - 1, False)


def local_stages(own, partner, w_first, w_second, skip):
    stages, local, _, size, _ = w_first.shape
    rows, width = own.shape
    first_steps = stages - skip
    steps = 1 + 2 * first_steps
    whole = pl.BlockSpec((rows, width), lambda t: (0, 0))
    w_block = (1, local, 2, size, size)
    flops = 4 * rows * size * width * steps
    return pl.pallas_call(
        functools.partial(local_kernel, first_steps),
        grid=(steps,),
        out_shape=jax.ShapeDtypeStruct((rows, width), own.dtype),
        in_specs=[
            whole,
            whole,
            pl.BlockSpec(w_block, lambda t: (jnp.minimum(t + skip - 1, stages - 1), 0, 0, 0, 0)),
            pl.BlockSpec(w_block, lambda t: (jnp.maximum(t - first_steps - 1, 0), 0, 0, 0, 0)),
        ],
        out_specs=whole,
        scratch_shapes=[pltpu.VMEM((rows, width), own.dtype)],
        compiler_params=pltpu.CompilerParams(dimension_semantics=("arbitrary",), vmem_limit_bytes=60 * 1024 * 1024),
        cost_estimate=pl.CostEstimate(flops=flops, bytes_accessed=6 * rows * width + 4 * rows * size * steps, transcendentals=0),
        name="local_stages",
    )(own, partner, w_first, w_second)


def solution(mesh):
    groups = mesh.shape["sp"]

    def swap(array, dev_step):
        return lax.ppermute(array, "sp", [(device, device ^ dev_step) for device in range(groups)])

    def device_program(signal, w_first, w_second):
        stages, local = w_first.shape[:2]
        rows, cols = signal.shape
        size = w_first.shape[-1]
        far = (2 ** (stages - 1)) // local
        near = far // 2
        width = WIDTH
        sent, source = [], signal
        for c in range(cols // width):
            chunk = source[:, c * width:(c + 1) * width]
            source, chunk = lax.optimization_barrier((source, chunk))
            sent.append(swap(chunk, far))
        late, done = [], ()
        for c, partner in enumerate(sent):
            act = cross_stage(signal, partner, w_first, 0, 0, local, width, (0, c), (0, 0), (rows, width), (0, 0), after=done)
            act = local_stages(act, swap(act, near), w_first, w_second, 2)
            partner = swap(act, near)
            pieces = LAST_PIECES if c == cols // width - 1 else (local,)
            first = 0
            for count in pieces:
                piece = cross_stage(act, partner, w_second, stages - 2, first, count, width, (first, 0), (first, 0),
                                    (count * size, width), (0, 0))
                late.append((c, first, count, piece, swap(piece, far)))
                first += count
            done = [piece]
        result = None
        for c, first, count, piece, partner in late:
            result = cross_stage(piece, partner, w_second, stages - 1, first, count, width, (0, 0), (0, 0), (rows, cols), (first, c),
                                 into=result, after=done)
        return result

    row_spec = P(("dp", "sp"), None)
    weight_spec = P(None, "sp", None, None, None)
    return jax.shard_map(device_program, mesh=mesh, in_specs=(row_spec, weight_spec, weight_spec), out_specs=row_spec, check_vma=False)
```

```python
import functools

import jax
import jax.numpy as jnp
from jax import lax
from jax.experimental import pallas as pl
from jax.experimental.pallas import tpu as pltpu
from jax.sharding import PartitionSpec as P


WIDTH = 256
LAST_PIECES = (32, 16, 8, 4, 4)
FIRST_PIECES = (8, 56)

ERFC_P = (2.326819970068386e-2, -1.387039388740657e-1, 3.687424674597105e-1, -5.824733027278666e-1, 6.210004621745983e-1,
          -4.944515323274145e-1, 3.404879937665872e-1, -2.741127028184656e-1, 5.638259427386472e-1)
ERFC_R = (-1.047766399936249e1, 1.297719955372516e1, -7.495518717768503e0, 2.921019019210786e0, -1.015265279202700e0,
          4.218463358204948e-1, -2.820767439740514e-1, 5.641895067754075e-1)


def horner(coeffs, y):
    total = jnp.full_like(y, coeffs[0])
    for c in coeffs[1:]:
        total = total * y + c
    return total


def gelu(x):
    a = x * (-(0.5 ** 0.5))
    mag = jnp.abs(a)
    far = jnp.maximum(mag, 1.0)
    q = 1.0 / far
    y = q * q
    poly = jnp.where(far < 2.0, horner(ERFC_P, y), horner(ERFC_R, y))
    tail = jnp.exp(-far * far) * q * poly
    tail = jnp.where(a < 0.0, 2.0 - tail, tail)
    return 0.5 * x * jnp.where(mag < 1.0, 1.0 - lax.erf(a), tail)


def mix(w_own, w_cross, z_own, z_cross):
    weights = jnp.concatenate([w_own, w_cross], axis=1)
    blocks = jnp.concatenate([z_own, z_cross], axis=0)
    return jnp.dot(weights, blocks, preferred_element_type=jnp.float32)


def cross_kernel(blocks, *refs):
    own, partner, w, out = refs[0], refs[1], refs[2], refs[-1]
    size = w.shape[-1]
    for b in range(blocks):
        rows = pl.ds(b * size, size)
        out[rows, :] = mix(w[0, b, 0], w[0, b, 1], own[rows, :], partner[rows, :]).astype(out.dtype)


def cross_stage(own, partner, weights, stage, first, count, width, own_at, partner_at, out_shape, out_at, into=None, after=()):
    size, blocks = weights.shape[-1], min(count, 8)
    any_space = pl.BlockSpec(memory_space=pl.ANY)

    def spec(at):
        row, col = at
        return pl.BlockSpec((blocks * size, width), lambda g: (row // blocks + g, col))

    operands = [own, partner, weights]
    in_specs = [
        spec(own_at),
        spec(partner_at),
        pl.BlockSpec((1, blocks, 2, size, size), lambda g: (stage, first // blocks + g, 0, 0, 0)),
    ]
    aliases = {}
    if into is not None:
        aliases = {len(operands): 0}
        operands.append(into)
    operands += after
    in_specs += [any_space] * (len(operands) - len(in_specs))
    rows = count * size
    return pl.pallas_call(
        functools.partial(cross_kernel, blocks),
        grid=(count // blocks,),
        out_shape=jax.ShapeDtypeStruct(out_shape, own.dtype),
        in_specs=in_specs,
        out_specs=spec(out_at),
        input_output_aliases=aliases,
        compiler_params=pltpu.CompilerParams(dimension_semantics=("arbitrary",)),
        cost_estimate=pl.CostEstimate(
            flops=4 * rows * size * width, bytes_accessed=6 * rows * width + 4 * rows * size, transcendentals=0),
        name="cross_stage",
    )(*operands)


def local_kernel(first_steps, own, partner, wf, ws, out, other):
    step = pl.program_id(0)
    local, size = wf.shape[1], wf.shape[-1]

    @pl.when(step == 0)
    def _():
        def body(b, carry):
            rows = pl.ds(pl.multiple_of(b * size, size), size)
            out[rows, :] = mix(wf[0, b, 0], wf[0, b, 1], own[rows, :], partner[rows, :]).astype(out.dtype)
            return carry

        lax.fori_loop(0, local, body, 0, unroll=8)

    def stage(w, src, dst, shift, act):
        def body(p, carry):
            i = lax.shift_left(lax.shift_right_logical(p, shift), shift + 1) + (p & (lax.shift_left(1, shift) - 1))
            j = i + lax.shift_left(1, shift)
            ri = pl.ds(pl.multiple_of(i * size, size), size)
            rj = pl.ds(pl.multiple_of(j * size, size), size)
            zi, zj = src[ri, :], src[rj, :]
            blocks = jnp.concatenate([zi, zj], axis=0)
            weights = jnp.concatenate([
                jnp.concatenate([w[0, i, 0], w[0, i, 1]], axis=1),
                jnp.concatenate([w[0, j, 1], w[0, j, 0]], axis=1),
            ], axis=0)
            mixed = jnp.dot(weights, blocks, preferred_element_type=jnp.float32)
            mixed = mixed.astype(dst.dtype)
            if act:
                mixed = gelu(mixed.astype(jnp.float32)).astype(dst.dtype)
            dst[ri, :] = mixed[:size]
            dst[rj, :] = mixed[size:]
            return carry

        lax.fori_loop(0, local // 2, body, 0, unroll=1 if act else 4)

    odd = (step % 2) == 1

    @pl.when(jnp.logical_and(jnp.logical_and(step >= 1, step < first_steps), odd))
    def _():
        stage(wf, out, other, first_steps - step, False)

    @pl.when(jnp.logical_and(jnp.logical_and(step >= 1, step < first_steps), jnp.logical_not(odd)))
    def _():
        stage(wf, other, out, first_steps - step, False)

    @pl.when(step == first_steps)
    def _():
        if first_steps % 2:
            stage(wf, out, other, 0, True)
        else:
            stage(wf, other, out, 0, True)

    @pl.when(jnp.logical_and(step > first_steps, odd))
    def _():
        stage(ws, out, other, step - first_steps - 1, False)

    @pl.when(jnp.logical_and(step > first_steps, jnp.logical_not(odd)))
    def _():
        stage(ws, other, out, step - first_steps - 1, False)


def local_stages(own, partner, w_first, w_second, skip):
    stages, local, _, size, _ = w_first.shape
    rows, width = own.shape
    first_steps = stages - skip
    steps = 1 + 2 * first_steps
    whole = pl.BlockSpec((rows, width), lambda t: (0, 0))
    w_block = (1, local, 2, size, size)
    flops = 4 * rows * size * width * steps
    return pl.pallas_call(
        functools.partial(local_kernel, first_steps),
        grid=(steps,),
        out_shape=jax.ShapeDtypeStruct((rows, width), own.dtype),
        in_specs=[
            whole,
            whole,
            pl.BlockSpec(w_block, lambda t: (jnp.minimum(t + skip - 1, stages - 1), 0, 0, 0, 0)),
            pl.BlockSpec(w_block, lambda t: (jnp.maximum(t - first_steps - 1, 0), 0, 0, 0, 0)),
        ],
        out_specs=whole,
        scratch_shapes=[pltpu.VMEM((rows, width), own.dtype)],
        compiler_params=pltpu.CompilerParams(dimension_semantics=("arbitrary",), vmem_limit_bytes=60 * 1024 * 1024),
        cost_estimate=pl.CostEstimate(flops=flops, bytes_accessed=6 * rows * width + 4 * rows * size * steps, transcendentals=0),
        name="local_stages",
    )(own, partner, w_first, w_second)


def solution(mesh):
    groups = mesh.shape["sp"]

    def swap(array, dev_step):
        return lax.ppermute(array, "sp", [(device, device ^ dev_step) for device in range(groups)])

    def device_program(signal, w_first, w_second):
        stages, local = w_first.shape[:2]
        rows, cols = signal.shape
        size = w_first.shape[-1]
        far = (2 ** (stages - 1)) // local
        near = far // 2
        width = WIDTH
        sent, source = [], signal
        for c in range(cols // width):
            pieces = FIRST_PIECES if c == 0 else (local,)
            first, parts = 0, []
            for count in pieces:
                piece = source[first * size:(first + count) * size, c * width:(c + 1) * width]
                source, piece = lax.optimization_barrier((source, piece))
                parts.append((first, count, swap(piece, far)))
                first += count
            sent.append(parts)
        late, done = [], ()
        for c, parts in enumerate(sent):
            act = None
            for first, count, partner in parts:
                act = cross_stage(signal, partner, w_first, 0, first, count, width, (first, c), (0, 0), (rows, width), (first, 0),
                                  into=act, after=done)
            act = local_stages(act, swap(act, near), w_first, w_second, 2)
            partner = swap(act, near)
            pieces = LAST_PIECES if c == cols // width - 1 else (local,)
            first = 0
            for count in pieces:
                piece = cross_stage(act, partner, w_second, stages - 2, first, count, width, (first, 0), (first, 0),
                                    (count * size, width), (0, 0))
                late.append((c, first, count, piece, swap(piece, far)))
                first += count
            done = [piece]
        result = None
        for c, first, count, piece, partner in late:
            result = cross_stage(piece, partner, w_second, stages - 1, first, count, width, (0, 0), (0, 0), (rows, cols), (first, c),
                                 into=result, after=done)
        return result

    row_spec = P(("dp", "sp"), None)
    weight_spec = P(None, "sp", None, None, None)
    return jax.shard_map(device_program, mesh=mesh, in_specs=(row_spec, weight_spec, weight_spec), out_specs=row_spec, check_vma=False)
```

```python
import functools
import math

import jax
import jax.numpy as jnp
from jax import lax
from jax.experimental import pallas as pl
from jax.experimental.pallas import tpu as pltpu
from jax.sharding import PartitionSpec as P


WIDTH = 256
LAST_PIECES = (32, 16, 8, 4, 2, 2)
FIRST_PIECES = (4, 60)
TAIL_BLOCKS = 4

ERFC_P = (2.326819970068386e-2, -1.387039388740657e-1, 3.687424674597105e-1, -5.824733027278666e-1, 6.210004621745983e-1,
          -4.944515323274145e-1, 3.404879937665872e-1, -2.741127028184656e-1, 5.638259427386472e-1)
ERFC_R = (-1.047766399936249e1, 1.297719955372516e1, -7.495518717768503e0, 2.921019019210786e0, -1.015265279202700e0,
          4.218463358204948e-1, -2.820767439740514e-1, 5.641895067754075e-1)


def horner(coeffs, y):
    total = jnp.full_like(y, coeffs[0])
    for c in coeffs[1:]:
        total = total * y + c
    return total


def gelu(x):
    a = x * (-(0.5 ** 0.5))
    mag = jnp.abs(a)
    far = jnp.maximum(mag, 1.0)
    q = 1.0 / far
    y = q * q
    poly = jnp.where(far < 2.0, horner(ERFC_P, y), horner(ERFC_R, y))
    tail = jnp.exp(-far * far) * q * poly
    tail = jnp.where(a < 0.0, 2.0 - tail, tail)
    return 0.5 * x * jnp.where(mag < 1.0, 1.0 - lax.erf(a), tail)


def mix(w_own, w_cross, z_own, z_cross):
    weights = jnp.concatenate([w_own, w_cross], axis=1)
    blocks = jnp.concatenate([z_own, z_cross], axis=0)
    return jnp.dot(weights, blocks, preferred_element_type=jnp.float32)


def cross_kernel(blocks, *refs):
    own, partner, w, out = refs[0], refs[1], refs[2], refs[-1]
    size = w.shape[-1]
    for b in range(blocks):
        rows = pl.ds(b * size, size)
        out[rows, :] = mix(w[0, b, 0], w[0, b, 1], own[rows, :], partner[rows, :]).astype(out.dtype)


def cross_stage(own, partner, weights, stage, first, count, width, own_at, partner_at, out_shape, out_at, into=None, after=()):
    size, blocks = weights.shape[-1], math.gcd(first, count, 8)
    any_space = pl.BlockSpec(memory_space=pl.ANY)

    def spec(at):
        row, col = at
        return pl.BlockSpec((blocks * size, width), lambda g: (row // blocks + g, col))

    operands = [own, partner, weights]
    in_specs = [
        spec(own_at),
        spec(partner_at),
        pl.BlockSpec((1, blocks, 2, size, size), lambda g: (stage, first // blocks + g, 0, 0, 0)),
    ]
    aliases = {}
    if into is not None:
        aliases = {len(operands): 0}
        operands.append(into)
    operands += after
    in_specs += [any_space] * (len(operands) - len(in_specs))
    rows = count * size
    return pl.pallas_call(
        functools.partial(cross_kernel, blocks),
        grid=(count // blocks,),
        out_shape=jax.ShapeDtypeStruct(out_shape, own.dtype),
        in_specs=in_specs,
        out_specs=spec(out_at),
        input_output_aliases=aliases,
        compiler_params=pltpu.CompilerParams(dimension_semantics=("arbitrary",)),
        cost_estimate=pl.CostEstimate(
            flops=4 * rows * size * width, bytes_accessed=6 * rows * width + 4 * rows * size, transcendentals=0),
        name="cross_stage",
    )(*operands)


def tail_kernel(count, first, col, own, partner, w, into, out, mixed, sem):
    del into
    size, width = w.shape[-1], own.shape[1]
    copies = []
    for b in range(count):
        rows = pl.ds(b * size, size)
        mixed[rows, :] = mix(w[b, 0], w[b, 1], own[rows, :], partner[rows, :]).astype(mixed.dtype)
        target = out.at[pl.ds((first + b) * size, size), pl.ds(col * width, width)]
        copies.append(pltpu.make_async_copy(mixed.at[rows, :], target, sem.at[b]))
        copies[-1].start()
    for copy in copies:
        copy.wait()


def tail_stage(own, partner, weights, first, count, col, into):
    size, width = weights.shape[-1], own.shape[1]
    vmem, any_space = pl.BlockSpec(memory_space=pltpu.VMEM), pl.BlockSpec(memory_space=pl.ANY)
    return pl.pallas_call(
        functools.partial(tail_kernel, count, first, col),
        out_shape=jax.ShapeDtypeStruct(into.shape, into.dtype),
        in_specs=[vmem, vmem, vmem, any_space],
        out_specs=any_space,
        scratch_shapes=[pltpu.VMEM((count * size, width), own.dtype), pltpu.SemaphoreType.DMA((count,))],
        input_output_aliases={3: 0},
        compiler_params=pltpu.CompilerParams(vmem_limit_bytes=4 * 1024 * 1024),
        cost_estimate=pl.CostEstimate(
            flops=4 * count * size * size * width, bytes_accessed=2 * count * size * width, transcendentals=0),
        name="tail_stage",
    )(own, partner, weights, into)


def local_kernel(first_steps, own, partner, wf, ws, out, other):
    step = pl.program_id(0)
    local, size = wf.shape[1], wf.shape[-1]

    @pl.when(step == 0)
    def _():
        def body(b, carry):
            rows = pl.ds(pl.multiple_of(b * size, size), size)
            out[rows, :] = mix(wf[0, b, 0], wf[0, b, 1], own[rows, :], partner[rows, :]).astype(out.dtype)
            return carry

        lax.fori_loop(0, local, body, 0, unroll=8)

    def stage(w, src, dst, shift, act):
        def body(p, carry):
            i = lax.shift_left(lax.shift_right_logical(p, shift), shift + 1) + (p & (lax.shift_left(1, shift) - 1))
            j = i + lax.shift_left(1, shift)
            ri = pl.ds(pl.multiple_of(i * size, size), size)
            rj = pl.ds(pl.multiple_of(j * size, size), size)
            zi, zj = src[ri, :], src[rj, :]
            blocks = jnp.concatenate([zi, zj], axis=0)
            weights = jnp.concatenate([
                jnp.concatenate([w[0, i, 0], w[0, i, 1]], axis=1),
                jnp.concatenate([w[0, j, 1], w[0, j, 0]], axis=1),
            ], axis=0)
            mixed = jnp.dot(weights, blocks, preferred_element_type=jnp.float32)
            mixed = mixed.astype(dst.dtype)
            if act:
                mixed = gelu(mixed.astype(jnp.float32)).astype(dst.dtype)
            dst[ri, :] = mixed[:size]
            dst[rj, :] = mixed[size:]
            return carry

        lax.fori_loop(0, local // 2, body, 0, unroll=1 if act else 4)

    odd = (step % 2) == 1

    @pl.when(jnp.logical_and(jnp.logical_and(step >= 1, step < first_steps), odd))
    def _():
        stage(wf, out, other, first_steps - step, False)

    @pl.when(jnp.logical_and(jnp.logical_and(step >= 1, step < first_steps), jnp.logical_not(odd)))
    def _():
        stage(wf, other, out, first_steps - step, False)

    @pl.when(step == first_steps)
    def _():
        if first_steps % 2:
            stage(wf, out, other, 0, True)
        else:
            stage(wf, other, out, 0, True)

    @pl.when(jnp.logical_and(step > first_steps, odd))
    def _():
        stage(ws, out, other, step - first_steps - 1, False)

    @pl.when(jnp.logical_and(step > first_steps, jnp.logical_not(odd)))
    def _():
        stage(ws, other, out, step - first_steps - 1, False)


def local_stages(own, partner, w_first, w_second, skip):
    stages, local, _, size, _ = w_first.shape
    rows, width = own.shape
    first_steps = stages - skip
    steps = 1 + 2 * first_steps
    whole = pl.BlockSpec((rows, width), lambda t: (0, 0))
    w_block = (1, local, 2, size, size)
    flops = 4 * rows * size * width * steps
    return pl.pallas_call(
        functools.partial(local_kernel, first_steps),
        grid=(steps,),
        out_shape=jax.ShapeDtypeStruct((rows, width), own.dtype),
        in_specs=[
            whole,
            whole,
            pl.BlockSpec(w_block, lambda t: (jnp.minimum(t + skip - 1, stages - 1), 0, 0, 0, 0)),
            pl.BlockSpec(w_block, lambda t: (jnp.maximum(t - first_steps - 1, 0), 0, 0, 0, 0)),
        ],
        out_specs=whole,
        scratch_shapes=[pltpu.VMEM((rows, width), own.dtype)],
        compiler_params=pltpu.CompilerParams(dimension_semantics=("arbitrary",), vmem_limit_bytes=60 * 1024 * 1024),
        cost_estimate=pl.CostEstimate(flops=flops, bytes_accessed=6 * rows * width + 4 * rows * size * steps, transcendentals=0),
        name="local_stages",
    )(own, partner, w_first, w_second)


def solution(mesh):
    groups = mesh.shape["sp"]

    def swap(array, dev_step):
        return lax.ppermute(array, "sp", [(device, device ^ dev_step) for device in range(groups)])

    def device_program(signal, w_first, w_second):
        stages, local = w_first.shape[:2]
        rows, cols = signal.shape
        size = w_first.shape[-1]
        far = (2 ** (stages - 1)) // local
        near = far // 2
        width = WIDTH
        sent, source = [], signal
        for c in range(cols // width):
            pieces = FIRST_PIECES if c == 0 else (local,)
            first, parts = 0, []
            for count in pieces:
                piece = source[first * size:(first + count) * size, c * width:(c + 1) * width]
                source, piece = lax.optimization_barrier((source, piece))
                parts.append((first, count, swap(piece, far)))
                first += count
            sent.append(parts)
        late, done = [], ()
        for c, parts in enumerate(sent):
            act = None
            for first, count, partner in parts:
                act = cross_stage(signal, partner, w_first, 0, first, count, width, (first, c), (0, 0), (rows, width), (first, 0),
                                  into=act, after=done)
            act = local_stages(act, swap(act, near), w_first, w_second, 2)
            partner = swap(act, near)
            pieces = LAST_PIECES if c == cols // width - 1 else (local,)
            first = 0
            for count in pieces:
                piece = cross_stage(act, partner, w_second, stages - 2, first, count, width, (first, 0), (first, 0),
                                    (count * size, width), (0, 0))
                late.append((c, first, count, piece, swap(piece, far)))
                first += count
            done = [piece]
        result = None
        for c, first, count, piece, partner in late:
            if count <= TAIL_BLOCKS:
                result = tail_stage(piece, partner, w_second[stages - 1, first:first + count], first, count, c, result)
                continue
            result = cross_stage(piece, partner, w_second, stages - 1, first, count, width, (0, 0), (0, 0), (rows, cols), (first, c),
                                 into=result, after=done)
        return result

    row_spec = P(("dp", "sp"), None)
    weight_spec = P(None, "sp", None, None, None)
    return jax.shard_map(device_program, mesh=mesh, in_specs=(row_spec, weight_spec, weight_spec), out_specs=row_spec, check_vma=False)
```

```python
import functools
import math

import jax
import jax.numpy as jnp
from jax import lax
from jax.experimental import pallas as pl
from jax.experimental.pallas import tpu as pltpu
from jax.sharding import PartitionSpec as P


WIDTH = 256
LAST_PIECES = (52, 8, 4)
FIRST_PIECES = (8, 56)
TAIL_BLOCKS = 8

ERFC_P = (2.326819970068386e-2, -1.387039388740657e-1, 3.687424674597105e-1, -5.824733027278666e-1, 6.210004621745983e-1,
          -4.944515323274145e-1, 3.404879937665872e-1, -2.741127028184656e-1, 5.638259427386472e-1)
ERFC_R = (-1.047766399936249e1, 1.297719955372516e1, -7.495518717768503e0, 2.921019019210786e0, -1.015265279202700e0,
          4.218463358204948e-1, -2.820767439740514e-1, 5.641895067754075e-1)


def horner(coeffs, y):
    total = jnp.full_like(y, coeffs[0])
    for c in coeffs[1:]:
        total = total * y + c
    return total


def gelu(x):
    a = x * (-(0.5 ** 0.5))
    mag = jnp.abs(a)
    far = jnp.maximum(mag, 1.0)
    q = 1.0 / far
    y = q * q
    poly = jnp.where(far < 2.0, horner(ERFC_P, y), horner(ERFC_R, y))
    tail = jnp.exp(-far * far) * q * poly
    tail = jnp.where(a < 0.0, 2.0 - tail, tail)
    return 0.5 * x * jnp.where(mag < 1.0, 1.0 - lax.erf(a), tail)


def mix(w_own, w_cross, z_own, z_cross):
    weights = jnp.concatenate([w_own, w_cross], axis=1)
    blocks = jnp.concatenate([z_own, z_cross], axis=0)
    return jnp.dot(weights, blocks, preferred_element_type=jnp.float32)


def cross_kernel(blocks, *refs):
    own, partner, w, out = refs[0], refs[1], refs[2], refs[-1]
    size = w.shape[-1]
    for b in range(blocks):
        rows = pl.ds(b * size, size)
        out[rows, :] = mix(w[0, b, 0], w[0, b, 1], own[rows, :], partner[rows, :]).astype(out.dtype)


def cross_stage(own, partner, weights, stage, first, count, width, own_at, partner_at, out_shape, out_at, into=None, after=()):
    size, blocks = weights.shape[-1], math.gcd(first, count, 8)
    any_space = pl.BlockSpec(memory_space=pl.ANY)

    def spec(at):
        row, col = at
        return pl.BlockSpec((blocks * size, width), lambda g: (row // blocks + g, col))

    operands = [own, partner, weights]
    in_specs = [
        spec(own_at),
        spec(partner_at),
        pl.BlockSpec((1, blocks, 2, size, size), lambda g: (stage, first // blocks + g, 0, 0, 0)),
    ]
    aliases = {}
    if into is not None:
        aliases = {len(operands): 0}
        operands.append(into)
    operands += after
    in_specs += [any_space] * (len(operands) - len(in_specs))
    rows = count * size
    return pl.pallas_call(
        functools.partial(cross_kernel, blocks),
        grid=(count // blocks,),
        out_shape=jax.ShapeDtypeStruct(out_shape, own.dtype),
        in_specs=in_specs,
        out_specs=spec(out_at),
        input_output_aliases=aliases,
        compiler_params=pltpu.CompilerParams(dimension_semantics=("arbitrary",)),
        cost_estimate=pl.CostEstimate(
            flops=4 * rows * size * width, bytes_accessed=6 * rows * width + 4 * rows * size, transcendentals=0),
        name="cross_stage",
    )(*operands)


def tail_kernel(count, first, col, own, partner, w, into, out, mixed, sem):
    del into
    size, width = w.shape[-1], own.shape[1]
    copies = []
    for b in range(count):
        rows = pl.ds(b * size, size)
        mixed[rows, :] = mix(w[b, 0], w[b, 1], own[rows, :], partner[rows, :]).astype(mixed.dtype)
        target = out.at[pl.ds((first + b) * size, size), pl.ds(col * width, width)]
        copies.append(pltpu.make_async_copy(mixed.at[rows, :], target, sem.at[b]))
        copies[-1].start()
    for copy in copies:
        copy.wait()


def tail_stage(own, partner, weights, first, count, col, into):
    size, width = weights.shape[-1], own.shape[1]
    vmem, any_space = pl.BlockSpec(memory_space=pltpu.VMEM), pl.BlockSpec(memory_space=pl.ANY)
    return pl.pallas_call(
        functools.partial(tail_kernel, count, first, col),
        out_shape=jax.ShapeDtypeStruct(into.shape, into.dtype),
        in_specs=[vmem, vmem, vmem, any_space],
        out_specs=any_space,
        scratch_shapes=[pltpu.VMEM((count * size, width), own.dtype), pltpu.SemaphoreType.DMA((count,))],
        input_output_aliases={3: 0},
        compiler_params=pltpu.CompilerParams(vmem_limit_bytes=4 * 1024 * 1024),
        cost_estimate=pl.CostEstimate(
            flops=4 * count * size * size * width, bytes_accessed=2 * count * size * width, transcendentals=0),
        name="tail_stage",
    )(own, partner, weights, into)


def local_kernel(first_steps, own, partner, wf, ws, out, other):
    step = pl.program_id(0)
    local, size = wf.shape[1], wf.shape[-1]

    @pl.when(step == 0)
    def _():
        def body(b, carry):
            rows = pl.ds(pl.multiple_of(b * size, size), size)
            out[rows, :] = mix(wf[0, b, 0], wf[0, b, 1], own[rows, :], partner[rows, :]).astype(out.dtype)
            return carry

        lax.fori_loop(0, local, body, 0, unroll=8)

    def stage(w, src, dst, shift, act):
        def body(p, carry):
            i = lax.shift_left(lax.shift_right_logical(p, shift), shift + 1) + (p & (lax.shift_left(1, shift) - 1))
            j = i + lax.shift_left(1, shift)
            ri = pl.ds(pl.multiple_of(i * size, size), size)
            rj = pl.ds(pl.multiple_of(j * size, size), size)
            zi, zj = src[ri, :], src[rj, :]
            blocks = jnp.concatenate([zi, zj], axis=0)
            weights = jnp.concatenate([
                jnp.concatenate([w[0, i, 0], w[0, i, 1]], axis=1),
                jnp.concatenate([w[0, j, 1], w[0, j, 0]], axis=1),
            ], axis=0)
            mixed = jnp.dot(weights, blocks, preferred_element_type=jnp.float32)
            mixed = mixed.astype(dst.dtype)
            if act:
                mixed = gelu(mixed.astype(jnp.float32)).astype(dst.dtype)
            dst[ri, :] = mixed[:size]
            dst[rj, :] = mixed[size:]
            return carry

        lax.fori_loop(0, local // 2, body, 0, unroll=1 if act else 4)

    odd = (step % 2) == 1

    @pl.when(jnp.logical_and(jnp.logical_and(step >= 1, step < first_steps), odd))
    def _():
        stage(wf, out, other, first_steps - step, False)

    @pl.when(jnp.logical_and(jnp.logical_and(step >= 1, step < first_steps), jnp.logical_not(odd)))
    def _():
        stage(wf, other, out, first_steps - step, False)

    @pl.when(step == first_steps)
    def _():
        if first_steps % 2:
            stage(wf, out, other, 0, True)
        else:
            stage(wf, other, out, 0, True)

    @pl.when(jnp.logical_and(step > first_steps, odd))
    def _():
        stage(ws, out, other, step - first_steps - 1, False)

    @pl.when(jnp.logical_and(step > first_steps, jnp.logical_not(odd)))
    def _():
        stage(ws, other, out, step - first_steps - 1, False)


def local_stages(own, partner, w_first, w_second, skip):
    stages, local, _, size, _ = w_first.shape
    rows, width = own.shape
    first_steps = stages - skip
    steps = 1 + 2 * first_steps
    whole = pl.BlockSpec((rows, width), lambda t: (0, 0))
    w_block = (1, local, 2, size, size)
    flops = 4 * rows * size * width * steps
    return pl.pallas_call(
        functools.partial(local_kernel, first_steps),
        grid=(steps,),
        out_shape=jax.ShapeDtypeStruct((rows, width), own.dtype),
        in_specs=[
            whole,
            whole,
            pl.BlockSpec(w_block, lambda t: (jnp.minimum(t + skip - 1, stages - 1), 0, 0, 0, 0)),
            pl.BlockSpec(w_block, lambda t: (jnp.maximum(t - first_steps - 1, 0), 0, 0, 0, 0)),
        ],
        out_specs=whole,
        scratch_shapes=[pltpu.VMEM((rows, width), own.dtype)],
        compiler_params=pltpu.CompilerParams(dimension_semantics=("arbitrary",), vmem_limit_bytes=60 * 1024 * 1024),
        cost_estimate=pl.CostEstimate(flops=flops, bytes_accessed=6 * rows * width + 4 * rows * size * steps, transcendentals=0),
        name="local_stages",
    )(own, partner, w_first, w_second)


def solution(mesh):
    groups = mesh.shape["sp"]

    def swap(array, dev_step):
        return lax.ppermute(array, "sp", [(device, device ^ dev_step) for device in range(groups)])

    def device_program(signal, w_first, w_second):
        stages, local = w_first.shape[:2]
        rows, cols = signal.shape
        size = w_first.shape[-1]
        far = (2 ** (stages - 1)) // local
        near = far // 2
        width = WIDTH
        sent, source = [], signal
        for c in range(cols // width):
            pieces = FIRST_PIECES if c == 0 else (local,)
            first, parts = 0, []
            for count in pieces:
                piece = source[first * size:(first + count) * size, c * width:(c + 1) * width]
                source, piece = lax.optimization_barrier((source, piece))
                parts.append((first, count, swap(piece, far)))
                first += count
            sent.append(parts)
        late, done = [], ()
        for c, parts in enumerate(sent):
            act = None
            for first, count, partner in parts:
                act = cross_stage(signal, partner, w_first, 0, first, count, width, (first, c), (0, 0), (rows, width), (first, 0),
                                  into=act, after=done)
            act = local_stages(act, swap(act, near), w_first, w_second, 2)
            partner = swap(act, near)
            pieces = LAST_PIECES if c == cols // width - 1 else (local,)
            first = 0
            for count in pieces:
                piece = cross_stage(act, partner, w_second, stages - 2, first, count, width, (first, 0), (first, 0),
                                    (count * size, width), (0, 0))
                late.append((c, first, count, piece, swap(piece, far)))
                first += count
            done = [piece]
        result = None
        for c, first, count, piece, partner in late:
            if count <= TAIL_BLOCKS:
                result = tail_stage(piece, partner, w_second[stages - 1, first:first + count], first, count, c, result)
                continue
            result = cross_stage(piece, partner, w_second, stages - 1, first, count, width, (0, 0), (0, 0), (rows, cols), (first, c),
                                 into=result, after=done)
        return result

    row_spec = P(("dp", "sp"), None)
    weight_spec = P(None, "sp", None, None, None)
    return jax.shard_map(device_program, mesh=mesh, in_specs=(row_spec, weight_spec, weight_spec), out_specs=row_spec, check_vma=False)
```

```python
import functools
import math

import jax
import jax.numpy as jnp
from jax import lax
from jax.experimental import pallas as pl
from jax.experimental.pallas import tpu as pltpu
from jax.sharding import PartitionSpec as P


WIDTH = 256
LAST_PIECES = (32, 16, 8, 4, 2, 2)
FIRST_PIECES = (8, 56)
TAIL_BLOCKS = 4

ERFC_P = (2.326819970068386e-2, -1.387039388740657e-1, 3.687424674597105e-1, -5.824733027278666e-1, 6.210004621745983e-1,
          -4.944515323274145e-1, 3.404879937665872e-1, -2.741127028184656e-1, 5.638259427386472e-1)
ERFC_R = (-1.047766399936249e1, 1.297719955372516e1, -7.495518717768503e0, 2.921019019210786e0, -1.015265279202700e0,
          4.218463358204948e-1, -2.820767439740514e-1, 5.641895067754075e-1)


def horner(coeffs, y):
    total = jnp.full_like(y, coeffs[0])
    for c in coeffs[1:]:
        total = total * y + c
    return total


def gelu(x):
    a = x * (-(0.5 ** 0.5))
    mag = jnp.abs(a)
    far = jnp.maximum(mag, 1.0)
    q = 1.0 / far
    y = q * q
    poly = jnp.where(far < 2.0, horner(ERFC_P, y), horner(ERFC_R, y))
    tail = jnp.exp(-far * far) * q * poly
    tail = jnp.where(a < 0.0, 2.0 - tail, tail)
    return 0.5 * x * jnp.where(mag < 1.0, 1.0 - lax.erf(a), tail)


def mix(w_own, w_cross, z_own, z_cross):
    weights = jnp.concatenate([w_own, w_cross], axis=1)
    blocks = jnp.concatenate([z_own, z_cross], axis=0)
    return jnp.dot(weights, blocks, preferred_element_type=jnp.float32)


def cross_kernel(blocks, *refs):
    own, partner, w, out = refs[0], refs[1], refs[2], refs[-1]
    size = w.shape[-1]

    def body(b, carry):
        rows = pl.ds(pl.multiple_of(b * size, size), size)
        out[rows, :] = mix(w[0, b, 0], w[0, b, 1], own[rows, :], partner[rows, :]).astype(out.dtype)
        return carry

    lax.fori_loop(0, blocks, body, 0, unroll=min(blocks, 8))


def cross_stage(own, partner, weights, stage, first, count, width, own_at, partner_at, out_shape, out_at, into=None, after=()):
    size, blocks = weights.shape[-1], math.gcd(first, count, 32)
    any_space = pl.BlockSpec(memory_space=pl.ANY)

    def spec(at):
        row, col = at
        return pl.BlockSpec((blocks * size, width), lambda g: (row // blocks + g, col))

    operands = [own, partner, weights]
    in_specs = [
        spec(own_at),
        spec(partner_at),
        pl.BlockSpec((1, blocks, 2, size, size), lambda g: (stage, first // blocks + g, 0, 0, 0)),
    ]
    aliases = {}
    if into is not None:
        aliases = {len(operands): 0}
        operands.append(into)
    operands += after
    in_specs += [any_space] * (len(operands) - len(in_specs))
    rows = count * size
    return pl.pallas_call(
        functools.partial(cross_kernel, blocks),
        grid=(count // blocks,),
        out_shape=jax.ShapeDtypeStruct(out_shape, own.dtype),
        in_specs=in_specs,
        out_specs=spec(out_at),
        input_output_aliases=aliases,
        compiler_params=pltpu.CompilerParams(dimension_semantics=("arbitrary",)),
        cost_estimate=pl.CostEstimate(
            flops=4 * rows * size * width, bytes_accessed=6 * rows * width + 4 * rows * size, transcendentals=0),
        name="cross_stage",
    )(*operands)


def tail_kernel(count, first, col, own, partner, w, into, out, mixed, sem):
    del into
    size, width = w.shape[-1], own.shape[1]
    copies = []
    for b in range(count):
        rows = pl.ds(b * size, size)
        mixed[rows, :] = mix(w[b, 0], w[b, 1], own[rows, :], partner[rows, :]).astype(mixed.dtype)
        target = out.at[pl.ds((first + b) * size, size), pl.ds(col * width, width)]
        copies.append(pltpu.make_async_copy(mixed.at[rows, :], target, sem.at[b]))
        copies[-1].start()
    for copy in copies:
        copy.wait()


def tail_stage(own, partner, weights, first, count, col, into):
    size, width = weights.shape[-1], own.shape[1]
    vmem, any_space = pl.BlockSpec(memory_space=pltpu.VMEM), pl.BlockSpec(memory_space=pl.ANY)
    return pl.pallas_call(
        functools.partial(tail_kernel, count, first, col),
        out_shape=jax.ShapeDtypeStruct(into.shape, into.dtype),
        in_specs=[vmem, vmem, vmem, any_space],
        out_specs=any_space,
        scratch_shapes=[pltpu.VMEM((count * size, width), own.dtype), pltpu.SemaphoreType.DMA((count,))],
        input_output_aliases={3: 0},
        compiler_params=pltpu.CompilerParams(vmem_limit_bytes=4 * 1024 * 1024),
        cost_estimate=pl.CostEstimate(
            flops=4 * count * size * size * width, bytes_accessed=2 * count * size * width, transcendentals=0),
        name="tail_stage",
    )(own, partner, weights, into)


def local_kernel(first_steps, own, partner, wf, ws, out, other):
    step = pl.program_id(0)
    local, size = wf.shape[1], wf.shape[-1]

    @pl.when(step == 0)
    def _():
        def body(b, carry):
            rows = pl.ds(pl.multiple_of(b * size, size), size)
            out[rows, :] = mix(wf[0, b, 0], wf[0, b, 1], own[rows, :], partner[rows, :]).astype(out.dtype)
            return carry

        lax.fori_loop(0, local, body, 0, unroll=8)

    def stage(w, src, dst, shift, act):
        def body(p, carry):
            i = lax.shift_left(lax.shift_right_logical(p, shift), shift + 1) + (p & (lax.shift_left(1, shift) - 1))
            j = i + lax.shift_left(1, shift)
            ri = pl.ds(pl.multiple_of(i * size, size), size)
            rj = pl.ds(pl.multiple_of(j * size, size), size)
            zi, zj = src[ri, :], src[rj, :]
            blocks = jnp.concatenate([zi, zj], axis=0)
            weights = jnp.concatenate([
                jnp.concatenate([w[0, i, 0], w[0, i, 1]], axis=1),
                jnp.concatenate([w[0, j, 1], w[0, j, 0]], axis=1),
            ], axis=0)
            mixed = jnp.dot(weights, blocks, preferred_element_type=jnp.float32)
            mixed = mixed.astype(dst.dtype)
            if act:
                mixed = gelu(mixed.astype(jnp.float32)).astype(dst.dtype)
            dst[ri, :] = mixed[:size]
            dst[rj, :] = mixed[size:]
            return carry

        lax.fori_loop(0, local // 2, body, 0, unroll=1 if act else 4)

    odd = (step % 2) == 1

    @pl.when(jnp.logical_and(jnp.logical_and(step >= 1, step < first_steps), odd))
    def _():
        stage(wf, out, other, first_steps - step, False)

    @pl.when(jnp.logical_and(jnp.logical_and(step >= 1, step < first_steps), jnp.logical_not(odd)))
    def _():
        stage(wf, other, out, first_steps - step, False)

    @pl.when(step == first_steps)
    def _():
        if first_steps % 2:
            stage(wf, out, other, 0, True)
        else:
            stage(wf, other, out, 0, True)

    @pl.when(jnp.logical_and(step > first_steps, odd))
    def _():
        stage(ws, out, other, step - first_steps - 1, False)

    @pl.when(jnp.logical_and(step > first_steps, jnp.logical_not(odd)))
    def _():
        stage(ws, other, out, step - first_steps - 1, False)


def local_stages(own, partner, w_first, w_second, skip):
    stages, local, _, size, _ = w_first.shape
    rows, width = own.shape
    first_steps = stages - skip
    steps = 1 + 2 * first_steps
    whole = pl.BlockSpec((rows, width), lambda t: (0, 0))
    w_block = (1, local, 2, size, size)
    flops = 4 * rows * size * width * steps
    return pl.pallas_call(
        functools.partial(local_kernel, first_steps),
        grid=(steps,),
        out_shape=jax.ShapeDtypeStruct((rows, width), own.dtype),
        in_specs=[
            whole,
            whole,
            pl.BlockSpec(w_block, lambda t: (jnp.minimum(t + skip - 1, stages - 1), 0, 0, 0, 0)),
            pl.BlockSpec(w_block, lambda t: (jnp.maximum(t - first_steps - 1, 0), 0, 0, 0, 0)),
        ],
        out_specs=whole,
        scratch_shapes=[pltpu.VMEM((rows, width), own.dtype)],
        compiler_params=pltpu.CompilerParams(dimension_semantics=("arbitrary",), vmem_limit_bytes=60 * 1024 * 1024),
        cost_estimate=pl.CostEstimate(flops=flops, bytes_accessed=6 * rows * width + 4 * rows * size * steps, transcendentals=0),
        name="local_stages",
    )(own, partner, w_first, w_second)


def solution(mesh):
    groups = mesh.shape["sp"]

    def swap(array, dev_step):
        return lax.ppermute(array, "sp", [(device, device ^ dev_step) for device in range(groups)])

    def device_program(signal, w_first, w_second):
        stages, local = w_first.shape[:2]
        rows, cols = signal.shape
        size = w_first.shape[-1]
        far = (2 ** (stages - 1)) // local
        near = far // 2
        width = WIDTH
        sent, source = [], signal
        for c in range(cols // width):
            pieces = FIRST_PIECES if c == 0 else (local,)
            first, parts = 0, []
            for count in pieces:
                piece = source[first * size:(first + count) * size, c * width:(c + 1) * width]
                source, piece = lax.optimization_barrier((source, piece))
                parts.append((first, count, swap(piece, far)))
                first += count
            sent.append(parts)
        late, done = [], ()
        for c, parts in enumerate(sent):
            act = None
            for first, count, partner in parts:
                act = cross_stage(signal, partner, w_first, 0, first, count, width, (first, c), (0, 0), (rows, width), (first, 0),
                                  into=act, after=done)
            act = local_stages(act, swap(act, near), w_first, w_second, 2)
            partner = swap(act, near)
            pieces = LAST_PIECES if c == cols // width - 1 else (local,)
            first = 0
            for count in pieces:
                piece = cross_stage(act, partner, w_second, stages - 2, first, count, width, (first, 0), (first, 0),
                                    (count * size, width), (0, 0))
                late.append((c, first, count, piece, swap(piece, far)))
                first += count
            done = [piece]
        result = None
        for c, first, count, piece, partner in late:
            if count <= TAIL_BLOCKS:
                result = tail_stage(piece, partner, w_second[stages - 1, first:first + count], first, count, c, result)
                continue
            result = cross_stage(piece, partner, w_second, stages - 1, first, count, width, (0, 0), (0, 0), (rows, cols), (first, c),
                                 into=result, after=done)
        return result

    row_spec = P(("dp", "sp"), None)
    weight_spec = P(None, "sp", None, None, None)
    return jax.shard_map(device_program, mesh=mesh, in_specs=(row_spec, weight_spec, weight_spec), out_specs=row_spec, check_vma=False)
```

```python
import functools
import math

import jax
import jax.numpy as jnp
from jax import lax
from jax.experimental import pallas as pl
from jax.experimental.pallas import tpu as pltpu
from jax.sharding import PartitionSpec as P


WIDTH = 256
LAST_PIECES = (32, 16, 8, 4, 2, 2)
FIRST_PIECES = (8, 56)
TAIL_BLOCKS = 4

ERFC_P = (2.326819970068386e-2, -1.387039388740657e-1, 3.687424674597105e-1, -5.824733027278666e-1, 6.210004621745983e-1,
          -4.944515323274145e-1, 3.404879937665872e-1, -2.741127028184656e-1, 5.638259427386472e-1)
ERFC_R = (-1.047766399936249e1, 1.297719955372516e1, -7.495518717768503e0, 2.921019019210786e0, -1.015265279202700e0,
          4.218463358204948e-1, -2.820767439740514e-1, 5.641895067754075e-1)


def horner(coeffs, y):
    total = jnp.full_like(y, coeffs[0])
    for c in coeffs[1:]:
        total = total * y + c
    return total


def gelu(x):
    a = x * (-(0.5 ** 0.5))
    mag = jnp.abs(a)
    far = jnp.maximum(mag, 1.0)
    q = 1.0 / far
    y = q * q
    poly = jnp.where(far < 2.0, horner(ERFC_P, y), horner(ERFC_R, y))
    tail = jnp.exp(-far * far) * q * poly
    tail = jnp.where(a < 0.0, 2.0 - tail, tail)
    return 0.5 * x * jnp.where(mag < 1.0, 1.0 - lax.erf(a), tail)


def mix(w_own, w_cross, z_own, z_cross):
    weights = jnp.concatenate([w_own, w_cross], axis=1)
    blocks = jnp.concatenate([z_own, z_cross], axis=0)
    return jnp.dot(weights, blocks, preferred_element_type=jnp.float32)


def take_kernel(row, rows, col, parts, source, out, held, sem_in, sem_out):
    width, step = out.shape[1], rows // parts
    ins = [pltpu.make_async_copy(source.at[pl.ds(row + p * step, step), pl.ds(col, width)], held.at[pl.ds(p * step, step), :], sem_in.at[p])
           for p in range(parts)]
    outs = [pltpu.make_async_copy(held.at[pl.ds(p * step, step), :], out.at[pl.ds(p * step, step), :], sem_out.at[p])
            for p in range(parts)]
    for copy in ins:
        copy.start()
    for p in range(parts):
        ins[p].wait()
        outs[p].start()
    for copy in outs:
        copy.wait()


def take(source, row, rows, col, width, parts):
    any_space = pl.BlockSpec(memory_space=pl.ANY)
    return pl.pallas_call(
        functools.partial(take_kernel, row, rows, col, parts),
        out_shape=jax.ShapeDtypeStruct((rows, width), source.dtype),
        in_specs=[any_space],
        out_specs=any_space,
        scratch_shapes=[pltpu.VMEM((rows, width), source.dtype), pltpu.SemaphoreType.DMA((parts,)), pltpu.SemaphoreType.DMA((parts,))],
        cost_estimate=pl.CostEstimate(flops=rows * width, bytes_accessed=4 * rows * width, transcendentals=0),
        name="take",
    )(source)


def cross_kernel(blocks, *refs):
    own, partner, w, out = refs[0], refs[1], refs[2], refs[-1]
    size = w.shape[-1]

    def body(b, carry):
        rows = pl.ds(pl.multiple_of(b * size, size), size)
        out[rows, :] = mix(w[0, b, 0], w[0, b, 1], own[rows, :], partner[rows, :]).astype(out.dtype)
        return carry

    lax.fori_loop(0, blocks, body, 0, unroll=min(blocks, 8))


def cross_stage(own, partner, weights, stage, first, count, width, own_at, partner_at, out_shape, out_at, into=None, after=()):
    size, blocks = weights.shape[-1], math.gcd(first, count, 32)
    any_space = pl.BlockSpec(memory_space=pl.ANY)

    def spec(at):
        row, col = at
        return pl.BlockSpec((blocks * size, width), lambda g: (row // blocks + g, col))

    operands = [own, partner, weights]
    in_specs = [
        spec(own_at),
        spec(partner_at),
        pl.BlockSpec((1, blocks, 2, size, size), lambda g: (stage, first // blocks + g, 0, 0, 0)),
    ]
    aliases = {}
    if into is not None:
        aliases = {len(operands): 0}
        operands.append(into)
    operands += after
    in_specs += [any_space] * (len(operands) - len(in_specs))
    rows = count * size
    return pl.pallas_call(
        functools.partial(cross_kernel, blocks),
        grid=(count // blocks,),
        out_shape=jax.ShapeDtypeStruct(out_shape, own.dtype),
        in_specs=in_specs,
        out_specs=spec(out_at),
        input_output_aliases=aliases,
        compiler_params=pltpu.CompilerParams(dimension_semantics=("arbitrary",)),
        cost_estimate=pl.CostEstimate(
            flops=4 * rows * size * width, bytes_accessed=6 * rows * width + 4 * rows * size, transcendentals=0),
        name="cross_stage",
    )(*operands)


def tail_kernel(count, first, col, own, partner, w, into, out, mixed, sem):
    del into
    size, width = w.shape[-1], own.shape[1]
    for b in range(count):
        rows = pl.ds(b * size, size)
        mixed[rows, :] = mix(w[b, 0], w[b, 1], own[rows, :], partner[rows, :]).astype(mixed.dtype)
    copy = pltpu.make_async_copy(mixed, out.at[pl.ds(first * size, count * size), pl.ds(col * width, width)], sem)
    copy.start()
    copy.wait()


def tail_stage(own, partner, weights, first, count, col, into):
    size, width = weights.shape[-1], own.shape[1]
    vmem, any_space = pl.BlockSpec(memory_space=pltpu.VMEM), pl.BlockSpec(memory_space=pl.ANY)
    return pl.pallas_call(
        functools.partial(tail_kernel, count, first, col),
        out_shape=jax.ShapeDtypeStruct(into.shape, into.dtype),
        in_specs=[vmem, vmem, vmem, any_space],
        out_specs=any_space,
        scratch_shapes=[pltpu.VMEM((count * size, width), own.dtype), pltpu.SemaphoreType.DMA],
        input_output_aliases={3: 0},
        compiler_params=pltpu.CompilerParams(vmem_limit_bytes=4 * 1024 * 1024),
        cost_estimate=pl.CostEstimate(
            flops=4 * count * size * size * width, bytes_accessed=2 * count * size * width, transcendentals=0),
        name="tail_stage",
    )(own, partner, weights, into)


def local_kernel(first_steps, own, partner, wf, ws, out, other):
    step = pl.program_id(0)
    local, size = wf.shape[1], wf.shape[-1]

    @pl.when(step == 0)
    def _():
        def body(b, carry):
            rows = pl.ds(pl.multiple_of(b * size, size), size)
            out[rows, :] = mix(wf[0, b, 0], wf[0, b, 1], own[rows, :], partner[rows, :]).astype(out.dtype)
            return carry

        lax.fori_loop(0, local, body, 0, unroll=8)

    def stage(w, src, dst, shift, act):
        def body(p, carry):
            i = lax.shift_left(lax.shift_right_logical(p, shift), shift + 1) + (p & (lax.shift_left(1, shift) - 1))
            j = i + lax.shift_left(1, shift)
            ri = pl.ds(pl.multiple_of(i * size, size), size)
            rj = pl.ds(pl.multiple_of(j * size, size), size)
            zi, zj = src[ri, :], src[rj, :]
            blocks = jnp.concatenate([zi, zj], axis=0)
            weights = jnp.concatenate([
                jnp.concatenate([w[0, i, 0], w[0, i, 1]], axis=1),
                jnp.concatenate([w[0, j, 1], w[0, j, 0]], axis=1),
            ], axis=0)
            mixed = jnp.dot(weights, blocks, preferred_element_type=jnp.float32)
            mixed = mixed.astype(dst.dtype)
            if act:
                mixed = gelu(mixed.astype(jnp.float32)).astype(dst.dtype)
            dst[ri, :] = mixed[:size]
            dst[rj, :] = mixed[size:]
            return carry

        lax.fori_loop(0, local // 2, body, 0, unroll=1 if act else 4)

    odd = (step % 2) == 1

    @pl.when(jnp.logical_and(jnp.logical_and(step >= 1, step < first_steps), odd))
    def _():
        stage(wf, out, other, first_steps - step, False)

    @pl.when(jnp.logical_and(jnp.logical_and(step >= 1, step < first_steps), jnp.logical_not(odd)))
    def _():
        stage(wf, other, out, first_steps - step, False)

    @pl.when(step == first_steps)
    def _():
        if first_steps % 2:
            stage(wf, out, other, 0, True)
        else:
            stage(wf, other, out, 0, True)

    @pl.when(jnp.logical_and(step > first_steps, odd))
    def _():
        stage(ws, out, other, step - first_steps - 1, False)

    @pl.when(jnp.logical_and(step > first_steps, jnp.logical_not(odd)))
    def _():
        stage(ws, other, out, step - first_steps - 1, False)


def local_stages(own, partner, w_first, w_second, skip):
    stages, local, _, size, _ = w_first.shape
    rows, width = own.shape
    first_steps = stages - skip
    steps = 1 + 2 * first_steps
    whole = pl.BlockSpec((rows, width), lambda t: (0, 0))
    w_block = (1, local, 2, size, size)
    flops = 4 * rows * size * width * steps
    return pl.pallas_call(
        functools.partial(local_kernel, first_steps),
        grid=(steps,),
        out_shape=jax.ShapeDtypeStruct((rows, width), own.dtype),
        in_specs=[
            whole,
            whole,
            pl.BlockSpec(w_block, lambda t: (jnp.minimum(t + skip - 1, stages - 1), 0, 0, 0, 0)),
            pl.BlockSpec(w_block, lambda t: (jnp.maximum(t - first_steps - 1, 0), 0, 0, 0, 0)),
        ],
        out_specs=whole,
        scratch_shapes=[pltpu.VMEM((rows, width), own.dtype)],
        compiler_params=pltpu.CompilerParams(dimension_semantics=("arbitrary",), vmem_limit_bytes=60 * 1024 * 1024),
        cost_estimate=pl.CostEstimate(flops=flops, bytes_accessed=6 * rows * width + 4 * rows * size * steps, transcendentals=0),
        name="local_stages",
    )(own, partner, w_first, w_second)


def solution(mesh):
    groups = mesh.shape["sp"]

    def swap(array, dev_step):
        return lax.ppermute(array, "sp", [(device, device ^ dev_step) for device in range(groups)])

    def device_program(signal, w_first, w_second):
        stages, local = w_first.shape[:2]
        rows, cols = signal.shape
        size = w_first.shape[-1]
        far = (2 ** (stages - 1)) // local
        near = far // 2
        width = WIDTH
        sent = []
        for c in range(cols // width):
            pieces = FIRST_PIECES if c == 0 else (local,)
            first, parts = 0, []
            for k, count in enumerate(pieces):
                if c == k == 0:
                    piece = signal[:count * size, :width]
                else:
                    piece = take(signal, first * size, count * size, c * width, width, 2)
                parts.append((first, count, swap(piece, far)))
                first += count
            sent.append(parts)
        late, done = [], ()
        for c, parts in enumerate(sent):
            act = None
            for first, count, partner in parts:
                act = cross_stage(signal, partner, w_first, 0, first, count, width, (first, c), (0, 0), (rows, width), (first, 0),
                                  into=act, after=done)
            act = local_stages(act, swap(act, near), w_first, w_second, 2)
            partner = swap(act, near)
            pieces = LAST_PIECES if c == cols // width - 1 else (local,)
            first = 0
            for count in pieces:
                piece = cross_stage(act, partner, w_second, stages - 2, first, count, width, (first, 0), (first, 0),
                                    (count * size, width), (0, 0))
                late.append((c, first, count, piece, swap(piece, far)))
                first += count
            done = [piece]
        result = None
        for c, first, count, piece, partner in late:
            if count <= TAIL_BLOCKS:
                result = tail_stage(piece, partner, w_second[stages - 1, first:first + count], first, count, c, result)
                continue
            result = cross_stage(piece, partner, w_second, stages - 1, first, count, width, (0, 0), (0, 0), (rows, cols), (first, c),
                                 into=result, after=done)
        return result

    row_spec = P(("dp", "sp"), None)
    weight_spec = P(None, "sp", None, None, None)
    return jax.shard_map(device_program, mesh=mesh, in_specs=(row_spec, weight_spec, weight_spec), out_specs=row_spec, check_vma=False)
```

```python
import functools

import jax
import jax.numpy as jnp
from jax import lax
from jax.experimental import pallas as pl
from jax.experimental.pallas import tpu as pltpu
from jax.sharding import PartitionSpec as P


WIDTH = 256
LAST_PIECES = (32, 16, 8, 4, 2, 2)
FIRST_PIECES = (4, 60)
TAIL_BLOCKS = 4

ERFC_P = (2.326819970068386e-2, -1.387039388740657e-1, 3.687424674597105e-1, -5.824733027278666e-1, 6.210004621745983e-1,
          -4.944515323274145e-1, 3.404879937665872e-1, -2.741127028184656e-1, 5.638259427386472e-1)
ERFC_R = (-1.047766399936249e1, 1.297719955372516e1, -7.495518717768503e0, 2.921019019210786e0, -1.015265279202700e0,
          4.218463358204948e-1, -2.820767439740514e-1, 5.641895067754075e-1)


def horner(coeffs, y):
    total = jnp.full_like(y, coeffs[0])
    for c in coeffs[1:]:
        total = total * y + c
    return total


def gelu(x):
    a = x * (-(0.5 ** 0.5))
    mag = jnp.abs(a)
    far = jnp.maximum(mag, 1.0)
    q = 1.0 / far
    y = q * q
    poly = jnp.where(far < 2.0, horner(ERFC_P, y), horner(ERFC_R, y))
    tail = jnp.exp(-far * far) * q * poly
    tail = jnp.where(a < 0.0, 2.0 - tail, tail)
    return 0.5 * x * jnp.where(mag < 1.0, 1.0 - lax.erf(a), tail)


def mix(w_own, w_cross, z_own, z_cross):
    weights = jnp.concatenate([w_own, w_cross], axis=1)
    blocks = jnp.concatenate([z_own, z_cross], axis=0)
    return jnp.dot(weights, blocks, preferred_element_type=jnp.float32)


def take_kernel(row, rows, col, parts, source, out, held, sem_in, sem_out):
    width, step = out.shape[1], rows // parts
    ins = [pltpu.make_async_copy(source.at[pl.ds(row + p * step, step), pl.ds(col, width)], held.at[pl.ds(p * step, step), :], sem_in.at[p])
           for p in range(parts)]
    outs = [pltpu.make_async_copy(held.at[pl.ds(p * step, step), :], out.at[pl.ds(p * step, step), :], sem_out.at[p])
            for p in range(parts)]
    for copy in ins:
        copy.start()
    for p in range(parts):
        ins[p].wait()
        outs[p].start()
    for copy in outs:
        copy.wait()


def take(source, row, rows, col, width, parts):
    any_space = pl.BlockSpec(memory_space=pl.ANY)
    return pl.pallas_call(
        functools.partial(take_kernel, row, rows, col, parts),
        out_shape=jax.ShapeDtypeStruct((rows, width), source.dtype),
        in_specs=[any_space],
        out_specs=any_space,
        scratch_shapes=[pltpu.VMEM((rows, width), source.dtype), pltpu.SemaphoreType.DMA((parts,)), pltpu.SemaphoreType.DMA((parts,))],
        cost_estimate=pl.CostEstimate(flops=rows * width, bytes_accessed=4 * rows * width, transcendentals=0),
        name="take",
    )(source)


def cross_kernel(blocks, *refs):
    own, partner, w, out = refs[0], refs[1], refs[2], refs[-1]
    size = w.shape[-1]

    def body(b, carry):
        rows = pl.ds(pl.multiple_of(b * size, size), size)
        out[rows, :] = mix(w[0, b, 0], w[0, b, 1], own[rows, :], partner[rows, :]).astype(out.dtype)
        return carry

    lax.fori_loop(0, blocks, body, 0, unroll=min(blocks, 8))


def cross_stage(own, partner, weights, stage, first, count, width, own_at, partner_at, out_shape, out_at, into=None, after=()):
    size = weights.shape[-1]
    blocks = max(b for b in range(1, 65) if count % b == 0)
    any_space = pl.BlockSpec(memory_space=pl.ANY)

    def spec(at):
        row, col = at
        return pl.BlockSpec((pl.Element(blocks * size), pl.Element(width)), lambda g: ((row + g * blocks) * size, col * width))

    operands = [own, partner, weights]
    w_shape = tuple(map(pl.Element, (1, blocks, 2, size, size)))
    in_specs = [
        spec(own_at),
        spec(partner_at),
        pl.BlockSpec(w_shape, lambda g: (stage, first + g * blocks, 0, 0, 0)),
    ]
    aliases = {}
    if into is not None:
        aliases = {len(operands): 0}
        operands.append(into)
    operands += after
    in_specs += [any_space] * (len(operands) - len(in_specs))
    rows = count * size
    return pl.pallas_call(
        functools.partial(cross_kernel, blocks),
        grid=(count // blocks,),
        out_shape=jax.ShapeDtypeStruct(out_shape, own.dtype),
        in_specs=in_specs,
        out_specs=spec(out_at),
        input_output_aliases=aliases,
        compiler_params=pltpu.CompilerParams(dimension_semantics=("arbitrary",)),
        cost_estimate=pl.CostEstimate(
            flops=4 * rows * size * width, bytes_accessed=6 * rows * width + 4 * rows * size, transcendentals=0),
        name="cross_stage",
    )(*operands)


def tail_kernel(count, first, col, own, partner, w, into, out, mixed, sem):
    del into
    size, width = w.shape[-1], own.shape[1]
    for b in range(count):
        rows = pl.ds(b * size, size)
        mixed[rows, :] = mix(w[b, 0], w[b, 1], own[rows, :], partner[rows, :]).astype(mixed.dtype)
    copy = pltpu.make_async_copy(mixed, out.at[pl.ds(first * size, count * size), pl.ds(col * width, width)], sem)
    copy.start()
    copy.wait()


def tail_stage(own, partner, weights, first, count, col, into):
    size, width = weights.shape[-1], own.shape[1]
    vmem, any_space = pl.BlockSpec(memory_space=pltpu.VMEM), pl.BlockSpec(memory_space=pl.ANY)
    return pl.pallas_call(
        functools.partial(tail_kernel, count, first, col),
        out_shape=jax.ShapeDtypeStruct(into.shape, into.dtype),
        in_specs=[vmem, vmem, vmem, any_space],
        out_specs=any_space,
        scratch_shapes=[pltpu.VMEM((count * size, width), own.dtype), pltpu.SemaphoreType.DMA],
        input_output_aliases={3: 0},
        compiler_params=pltpu.CompilerParams(vmem_limit_bytes=4 * 1024 * 1024),
        cost_estimate=pl.CostEstimate(
            flops=4 * count * size * size * width, bytes_accessed=2 * count * size * width, transcendentals=0),
        name="tail_stage",
    )(own, partner, weights, into)


def local_kernel(first_steps, own, partner, wf, ws, out, other):
    step = pl.program_id(0)
    local, size = wf.shape[1], wf.shape[-1]

    @pl.when(step == 0)
    def _():
        def body(b, carry):
            rows = pl.ds(pl.multiple_of(b * size, size), size)
            out[rows, :] = mix(wf[0, b, 0], wf[0, b, 1], own[rows, :], partner[rows, :]).astype(out.dtype)
            return carry

        lax.fori_loop(0, local, body, 0, unroll=8)

    def stage(w, src, dst, shift, act):
        def body(p, carry):
            i = lax.shift_left(lax.shift_right_logical(p, shift), shift + 1) + (p & (lax.shift_left(1, shift) - 1))
            j = i + lax.shift_left(1, shift)
            ri = pl.ds(pl.multiple_of(i * size, size), size)
            rj = pl.ds(pl.multiple_of(j * size, size), size)
            zi, zj = src[ri, :], src[rj, :]
            blocks = jnp.concatenate([zi, zj], axis=0)
            weights = jnp.concatenate([
                jnp.concatenate([w[0, i, 0], w[0, i, 1]], axis=1),
                jnp.concatenate([w[0, j, 1], w[0, j, 0]], axis=1),
            ], axis=0)
            mixed = jnp.dot(weights, blocks, preferred_element_type=jnp.float32)
            mixed = mixed.astype(dst.dtype)
            if act:
                mixed = gelu(mixed.astype(jnp.float32)).astype(dst.dtype)
            dst[ri, :] = mixed[:size]
            dst[rj, :] = mixed[size:]
            return carry

        lax.fori_loop(0, local // 2, body, 0, unroll=1 if act else 4)

    odd = (step % 2) == 1

    @pl.when(jnp.logical_and(jnp.logical_and(step >= 1, step < first_steps), odd))
    def _():
        stage(wf, out, other, first_steps - step, False)

    @pl.when(jnp.logical_and(jnp.logical_and(step >= 1, step < first_steps), jnp.logical_not(odd)))
    def _():
        stage(wf, other, out, first_steps - step, False)

    @pl.when(step == first_steps)
    def _():
        if first_steps % 2:
            stage(wf, out, other, 0, True)
        else:
            stage(wf, other, out, 0, True)

    @pl.when(jnp.logical_and(step > first_steps, odd))
    def _():
        stage(ws, out, other, step - first_steps - 1, False)

    @pl.when(jnp.logical_and(step > first_steps, jnp.logical_not(odd)))
    def _():
        stage(ws, other, out, step - first_steps - 1, False)


def local_stages(own, partner, w_first, w_second, skip):
    stages, local, _, size, _ = w_first.shape
    rows, width = own.shape
    first_steps = stages - skip
    steps = 1 + 2 * first_steps
    whole = pl.BlockSpec((rows, width), lambda t: (0, 0))
    w_block = (1, local, 2, size, size)
    flops = 4 * rows * size * width * steps
    return pl.pallas_call(
        functools.partial(local_kernel, first_steps),
        grid=(steps,),
        out_shape=jax.ShapeDtypeStruct((rows, width), own.dtype),
        in_specs=[
            whole,
            whole,
            pl.BlockSpec(w_block, lambda t: (jnp.minimum(t + skip - 1, stages - 1), 0, 0, 0, 0)),
            pl.BlockSpec(w_block, lambda t: (jnp.maximum(t - first_steps - 1, 0), 0, 0, 0, 0)),
        ],
        out_specs=whole,
        scratch_shapes=[pltpu.VMEM((rows, width), own.dtype)],
        compiler_params=pltpu.CompilerParams(dimension_semantics=("arbitrary",), vmem_limit_bytes=60 * 1024 * 1024),
        cost_estimate=pl.CostEstimate(flops=flops, bytes_accessed=6 * rows * width + 4 * rows * size * steps, transcendentals=0),
        name="local_stages",
    )(own, partner, w_first, w_second)


def solution(mesh):
    groups = mesh.shape["sp"]

    def swap(array, dev_step):
        return lax.ppermute(array, "sp", [(device, device ^ dev_step) for device in range(groups)])

    def device_program(signal, w_first, w_second):
        stages, local = w_first.shape[:2]
        rows, cols = signal.shape
        size = w_first.shape[-1]
        far = (2 ** (stages - 1)) // local
        near = far // 2
        width = WIDTH
        sent = []
        for c in range(cols // width):
            pieces = FIRST_PIECES if c == 0 else (local,)
            first, parts = 0, []
            for k, count in enumerate(pieces):
                if c == k == 0:
                    piece = signal[:count * size, :width]
                else:
                    piece = take(signal, first * size, count * size, c * width, width, 2)
                parts.append((first, count, swap(piece, far)))
                first += count
            sent.append(parts)
        late, done = [], ()
        for c, parts in enumerate(sent):
            act = None
            for first, count, partner in parts:
                act = cross_stage(signal, partner, w_first, 0, first, count, width, (first, c), (0, 0), (rows, width), (first, 0),
                                  into=act, after=done)
            act = local_stages(act, swap(act, near), w_first, w_second, 2)
            partner = swap(act, near)
            pieces = LAST_PIECES if c == cols // width - 1 else (local,)
            first = 0
            for count in pieces:
                piece = cross_stage(act, partner, w_second, stages - 2, first, count, width, (first, 0), (first, 0),
                                    (count * size, width), (0, 0))
                late.append((c, first, count, piece, swap(piece, far)))
                first += count
            done = [piece]
        result = None
        for c, first, count, piece, partner in late:
            if count <= TAIL_BLOCKS:
                result = tail_stage(piece, partner, w_second[stages - 1, first:first + count], first, count, c, result)
                continue
            result = cross_stage(piece, partner, w_second, stages - 1, first, count, width, (0, 0), (0, 0), (rows, cols), (first, c),
                                 into=result, after=done)
        return result

    row_spec = P(("dp", "sp"), None)
    weight_spec = P(None, "sp", None, None, None)
    return jax.shard_map(device_program, mesh=mesh, in_specs=(row_spec, weight_spec, weight_spec), out_specs=row_spec, check_vma=False)
```
